16 devices in a mesh: dp: 4 (over y, z, core), sp: 4 (over x).
Axes of the slice: x: 4, y: 2, z: 1, core: 2. Of those that a mesh axis runs over, the one named last changes fastest.
The devices are a block of a 4x4x8 slice.
Arguments:
- x: bfloat16 [16384, 4096], P(('dp', 'sp')), parts along dimension 0
- gain: bfloat16 [4096], replicated
- wq: bfloat16 [4096, 4096], P('sp')
- wk: bfloat16 [4096, 256], P('sp')
- wv: bfloat16 [4096, 256], P('sp')
- wo: bfloat16 [4096, 4096], P('sp')
Outputs:
- output: bfloat16 [16384, 4096], P(('dp', 'sp')), parts along dimension 0
There are 4 independent parts. The reference program is written for one: setup_inputs(seed, part) draws one part's arguments, and reference() takes and returns one part's arrays. A program takes and returns all parts, laid end to end along the dimension named above; an argument that names none is the same for every part.
All inputs are finite; a program needn't handle non-finite values.
Results may differ from the reference program's by a relative error of at most 0.012.
Values are sent between devices in bfloat16 or wider.
A program may use at most 768 MiB of HBM per device.

```python
import jax
import jax.numpy as jnp
from jax import lax

ROWS = 4096
D = 4096
HEADS = 32
KV_HEADS = 2
HEAD = 128
THETA = 10000


def setup_inputs(seed: int = 0, part: int = 0) -> dict:
    kx, kn, kq, kk, kv, ko = jax.random.split(jax.random.key(seed), 6)

    def weights(key, rows, columns):
        return jax.random.normal(key, (rows, columns), jnp.float32) * rows**-0.5

    drawn = {
        "x": jax.random.normal(jax.random.fold_in(kx, part), (ROWS, D), jnp.float32),
        "gain": 1 + 0.1 * jax.random.normal(kn, (D,), jnp.float32),
        "wq": 2 * weights(kq, D, HEADS * HEAD),
        "wk": 2 * weights(kk, D, KV_HEADS * HEAD),
        "wv": 4 * weights(kv, D, KV_HEADS * HEAD),
        "wo": weights(ko, HEADS * HEAD, D),
    }
    return {k: v.astype(jnp.bfloat16) for k, v in drawn.items()}


def normed(x, gain):
    wide = x.astype(jnp.float32)
    scale = lax.rsqrt(jnp.mean(wide * wide, -1, keepdims=True) + 1e-6)
    return (wide * scale * gain.astype(jnp.float32)).astype(jnp.bfloat16)


def turned(t, place, theta):
    half = t.shape[-1] // 2
    angle = place.astype(jnp.float32)[:, None] * theta ** (-jnp.arange(half, dtype=jnp.float32) / half)
    cos, sin = jnp.cos(angle)[:, None], jnp.sin(angle)[:, None]
    a, b = t[..., :half].astype(jnp.float32), t[..., half:].astype(jnp.float32)
    return jnp.concatenate([a * cos - b * sin, b * cos + a * sin], -1).astype(jnp.bfloat16)


def matmul(a, w):
    return jnp.dot(a, w, preferred_element_type=jnp.float32).astype(jnp.bfloat16)


def einsum(form, a, b):
    return jnp.einsum(form, a.astype(jnp.float32), b.astype(jnp.float32))


def attention(q, k, v):
    scores = einsum("tgsd,ugd->gstu", q, k) * q.shape[-1] ** -0.5
    token = jnp.arange(q.shape[0])
    scores = jnp.where(token[:, None] >= token, scores, -jnp.inf)
    weights = jax.nn.softmax(scores, -1).astype(jnp.bfloat16)
    return einsum("gstu,ugd->tgsd", weights, v).astype(jnp.bfloat16)


def reference(x, gain, wq, wk, wv, wo):
    a, place = normed(x, gain), jnp.arange(ROWS)
    q = turned(matmul(a, wq).reshape(ROWS, HEADS, HEAD), place, THETA).reshape(ROWS, KV_HEADS, -1, HEAD)
    k = turned(matmul(a, wk).reshape(ROWS, KV_HEADS, HEAD), place, THETA)
    v = matmul(a, wv).reshape(ROWS, KV_HEADS, HEAD)
    seen = attention(q, k, v).reshape(ROWS, HEADS * HEAD)
    return (x.astype(jnp.float32) + jnp.dot(seen, wo, preferred_element_type=jnp.float32)).astype(jnp.bfloat16)
```

```python
import functools

import jax
import jax.numpy as jnp
from jax import lax
from jax.experimental import pallas as pl
from jax.experimental.pallas import tpu as pltpu
from jax.sharding import PartitionSpec as P

HEAD = 128
THETA = 10000
NEG = -1e30
HIDDEN = 2 * NEG
LOG2E = 1.4426950408889634
VMEM = 67043328
MESH = pl.DeviceIdType.MESH

HEADS = 8
COLS = HEADS * HEAD
BQ = 256
BK = 512
STRIP = 512
DV = HEAD + 16

XR, XL, RR, RL, Q1, Q2, Q3, D1, D2, D3, D4, D5, D6 = range(13)
KR, KL, VR, VL, KRR, VLL = range(6)


def _dot(a, b, ca, cb):
    return lax.dot_general(a, b, (((ca,), (cb,)), ((), ())), preferred_element_type=jnp.float32)


def _kernel(chunks, kv_heads, cos_ref, sin_ref, gain_ref, x_ref, wq_ref, wk_ref, wv_ref, wo_ref, seen_ref, wof_ref,
            a_s, wq_s, wkv_s, k_s, v_s, q_s, xin, sout, top_s, mix_s, ss, rs, kss, krs, xsem, osem, lsem, wsem, bsem):
    own = x_ref.shape[0]
    deep = wq_ref.shape[0]
    dp, me = lax.axis_index("dp"), lax.axis_index("sp")
    n = lax.axis_size("sp")
    right, left, far = lax.rem(me + 1, n), lax.rem(me + n - 1, n), lax.rem(me + 2, n)
    core = lax.rem(dp, 2)
    p = lax.rem(lax.div(dp, 2), 2)
    mate = {"dp": dp + 1 - 2 * core, "sp": me}
    pair = {"dp": dp + 2 - 4 * p, "sp": me}
    to_right, to_left = {"dp": dp, "sp": right}, {"dp": dp, "sp": left}
    half, quarter = deep // 2, deep // 8

    barrier = pltpu.get_barrier_semaphore()
    for other in (mate, pair, to_right, to_left):
        pl.semaphore_signal(barrier, inc=1, device_id=other, device_id_type=MESH)
    pl.semaphore_wait(barrier, 4)

    kvw = wk_ref.shape[1]
    rounds = 1 + 2 * chunks

    def place(r, shard, row, size):
        at = pl.ds(pl.multiple_of(shard * deep + row, 128), size)
        if r == 0:
            return wkv_s.at[at, :]
        if r <= chunks:
            return wq_s.at[r - 1, at, :]
        return wof_ref.at[at, pl.ds((r - 1 - chunks) * COLS, COLS)]

    def source(r, row, size):
        if r == 0:
            return place(r, me, row, size)
        at = pl.ds(pl.multiple_of(row, 128), size)
        c = (r - 1) % chunks
        return (wq_ref if r <= chunks else wo_ref).at[at, pl.ds(c * COLS, COLS)]

    def copy(r, kind, arriving=False):
        b, pp = core * half, p
        if arriving and kind in (Q1, Q2, Q3):
            pp = 1 - p
        if arriving and kind >= D1:
            b = (1 - core) * half
        row, size, shard, to = {
            XR: (b + pp * quarter, 3 * quarter, left if arriving else me, to_right),
            XL: (b + pp * quarter, 3 * quarter, right if arriving else me, to_left),
            RR: (b + (1 + pp) * quarter, quarter, far if arriving else left, to_right),
            RL: (b + 3 * pp * quarter, quarter, far if arriving else right, to_left),
            Q1: (b + 3 * pp * quarter, quarter, left, pair),
            Q2: (b + 3 * pp * quarter, quarter, right, pair),
            Q3: (b + pp * 2 * quarter, 2 * quarter, far, pair),
            D1: (b + pp * quarter, 3 * quarter, left, mate),
            D2: (b + pp * quarter, 3 * quarter, right, mate),
            D3: (b + 3 * (1 - pp) * quarter, quarter, left, mate),
            D4: (b + 3 * (1 - pp) * quarter, quarter, right, mate),
            D5: (b + pp * 2 * quarter, 2 * quarter, far, mate),
            D6: (b + (1 - pp) * 2 * quarter, 2 * quarter, far, mate),
        }[kind]
        dst = place(r, shard, row, size)
        src = source(r, row, size) if kind in (XR, XL) and not arriving else dst
        return pltpu.make_async_remote_copy(src_ref=src, dst_ref=dst, send_sem=ss.at[r, kind], recv_sem=rs.at[r, kind],
                                            device_id=to, device_id_type=MESH)

    def start(r, *kinds):
        for kind in kinds:
            copy(r, kind).start()

    def arrive(r, *kinds):
        for kind in kinds:
            copy(r, kind, True).wait_recv()

    def sent(r):
        for kind in range(13):
            copy(r, kind).wait_send()

    def s0(r):
        start(r, XR, XL)

    def s1(r):
        arrive(r, XR)
        start(r, RR, Q1, D1)
        arrive(r, XL)
        start(r, RL, Q2, D2)

    def s2(r):
        arrive(r, RR, RL)
        start(r, Q3, D5)
        arrive(r, Q1, Q2)
        start(r, D3, D4)

    def s3(r):
        arrive(r, Q3)
        start(r, D6)

    def s4(r):
        arrive(r, D1, D2, D3, D4, D5, D6)

    def kv_copy(kind, arriving=False):
        shard = {KR: left if arriving else me, KL: right if arriving else me, VR: left if arriving else me,
                 VL: right if arriving else me, KRR: far if arriving else left, VLL: far if arriving else right}[kind]
        to = to_right if kind in (KR, VR, KRR) else to_left
        at = pl.ds(pl.multiple_of(shard * own, 128), own)
        ref = k_s.at[:, at, :] if kind in (KR, KL, KRR) else v_s.at[:, pl.ds(0, HEAD), at]
        return pltpu.make_async_remote_copy(src_ref=ref, dst_ref=ref, send_sem=kss.at[kind], recv_sem=krs.at[kind],
                                            device_id=to, device_id_type=MESH)

    mine = pl.ds(pl.multiple_of(me * deep, 128), deep)
    wk_in = pltpu.make_async_copy(wk_ref, wkv_s.at[mine, pl.ds(0, kvw)], lsem.at[0])
    wv_in = pltpu.make_async_copy(wv_ref, wkv_s.at[mine, pl.ds(kvw, kvw)], lsem.at[1])
    wk_in.start()
    wv_in.start()
    rows = xin.shape[1]
    x_in = [pltpu.make_async_copy(x_ref.at[pl.ds(i * rows, rows), :], xin.at[i % 2], xsem.at[i % 2]) for i in range(own // rows)]
    x_in[0].start()
    x_in[1].start()
    wk_in.wait()
    wv_in.wait()
    s0(0)
    wq_in = [pltpu.make_async_copy(wq_ref.at[:, pl.ds(c * COLS, COLS)], wq_s.at[c, mine, :], wsem.at[c]) for c in range(chunks)]
    for w in wq_in:
        w.start()

    for i, block in enumerate(x_in):
        block.wait()
        wide = xin[i % 2].astype(jnp.float32)
        scale = lax.rsqrt(jnp.mean(wide * wide, -1, keepdims=True) + 1e-6)
        a_s[i * rows : (i + 1) * rows, :] = (wide * scale * gain_ref[...].astype(jnp.float32)).astype(jnp.bfloat16)
        if i + 2 < len(x_in):
            x_in[i + 2].start()
    for h in range(kv_heads):
        v_s[h, HEAD:, :] = jnp.ones((DV - HEAD, v_s.shape[2]), jnp.bfloat16)

    s1(0)
    s0(1)
    s2(0)
    s3(0)
    s4(0)

    def turn(t, at):
        wide = t.astype(jnp.bfloat16).astype(jnp.float32)
        return (wide * cos_ref[at, :] + pltpu.roll(wide, HEAD // 2, 1) * sin_ref[at, :]).astype(jnp.bfloat16)

    def keys_values(i, _):
        at = pl.ds(pl.multiple_of(i * BQ, BQ), BQ)
        there = pl.ds(pl.multiple_of(me * own + i * BQ, BQ), BQ)
        kv = _dot(a_s[at, :], wkv_s[...], 1, 0)
        for h in range(kv_heads):
            k_s[h, there, :] = turn(kv[:, h * HEAD : (h + 1) * HEAD], at)
            v_s[h, :HEAD, there] = kv[:, kvw + h * HEAD : kvw + (h + 1) * HEAD].astype(jnp.bfloat16).T
        return _

    lax.fori_loop(0, own // BQ, keys_values, None)

    s1(1)
    for kind in (KR, KL, VR, VL):
        kv_copy(kind).start()
    s0(2)
    s2(1)
    kv_copy(KR, True).wait_recv()
    kv_copy(KRR).start()
    kv_copy(VL, True).wait_recv()
    kv_copy(VLL).start()
    s0(3)
    s3(1)
    s4(1)
    for kind in (KL, VR, KRR, VLL):
        kv_copy(kind, True).wait_recv()

    group = 2
    tall = own // 2

    def project(c):
        def tile(i, _):
            m, j = lax.div(i, HEADS // group), lax.rem(i, HEADS // group)
            at = pl.ds(pl.multiple_of(m * tall, tall), tall)
            cols = pl.ds(pl.multiple_of(j * group * HEAD, group * HEAD), group * HEAD)
            q = _dot(a_s[at, :], wq_s[c, :, cols], 1, 0)
            for h in range(group):
                q_s[j * group + h, at, :] = turn(q[:, h * HEAD : (h + 1) * HEAD], at)
            return _

        lax.fori_loop(0, 2 * (HEADS // group), tile, None)

    e = HEAD**-0.5 * LOG2E
    wide = HEADS * BQ
    strips = list(range(0, wide, STRIP))

    def attend(c, qb):
        g = lax.div(c * kv_heads, chunks)
        first = me * own + qb * BQ
        q = q_s[:, pl.ds(pl.multiple_of(qb * BQ, BQ), BQ), :].reshape(wide, HEAD)
        top_s[...] = jnp.full(top_s.shape, NEG, jnp.float32)
        mix_s[...] = jnp.zeros(mix_s.shape, jnp.float32)

        def block(j, masked):
            here = pl.ds(pl.multiple_of(j * BK, BK), BK)
            keys, values = k_s[g, here, :], v_s[g, :, here]
            scores = [_dot(keys, q[at : at + STRIP], 1, 1) for at in strips]
            if masked:
                gap = lax.rem(lax.broadcasted_iota(jnp.int32, (BK, STRIP), 1), BQ) - lax.broadcasted_iota(jnp.int32, (BK, STRIP), 0)
                ok = gap >= j * BK - first
            weights, keeps = [], []
            for at, s in zip(strips, scores):
                if masked:
                    s = jnp.where(ok, s, HIDDEN)
                old = top_s[:, at : at + STRIP]
                top = jnp.maximum(old, s.max(axis=0, keepdims=True))
                top_s[:, at : at + STRIP] = top
                weights.append(jnp.exp2((s - top) * e).astype(jnp.bfloat16))
                keeps.append(jnp.exp2((old - top) * e))
            for at, w, keep in zip(strips, weights, keeps):
                mix_s[:, at : at + STRIP] = mix_s[:, at : at + STRIP] * keep + _dot(values, w, 1, 0)

        whole, last = lax.div(first + 1, BK), lax.div(first + BQ - 1 + BK, BK)
        lax.fori_loop(0, whole, lambda j, _: block(j, False), None)
        lax.fori_loop(whole, last, lambda j, _: block(j, True), None)

    steps = own // BQ

    def out_copy(t):
        c, qb, slot = lax.div(t, steps), lax.rem(t, steps), lax.rem(t, 2)
        return pltpu.make_async_copy(sout.at[slot], seen_ref.at[pl.ds(pl.multiple_of(qb * BQ, BQ), BQ), pl.ds(pl.multiple_of(c * COLS, COLS), COLS)],
                                     osem.at[slot])

    bounce = [pltpu.make_async_copy(wo_ref.at[:, pl.ds(c * COLS, COLS)], wq_s.at[0, pl.ds(c * deep, deep), :], bsem.at[c]) for c in range(chunks)]
    settle = [pltpu.make_async_copy(wq_s.at[0, pl.ds(c * deep, deep), :], wof_ref.at[mine, pl.ds(c * COLS, COLS)], lsem.at[c])
              for c in range(chunks)]

    todo = {t: [] for t in range(chunks * steps)}
    for i, r in enumerate(range(2, rounds)):
        todo[2 * i].append(functools.partial(s1, r))
        if r + 2 < rounds:
            todo[2 * i].append(functools.partial(s0, r + 2))
        todo[2 * i + 1].append(functools.partial(s2, r))
        todo[2 * i + 3].append(functools.partial(s3, r))
    todo[0].append(wq_in[0].wait)
    for c in range(1, chunks):
        todo[steps * c] += [functools.partial(s4, 1 + c), wq_in[c].wait]

    def before():
        sent(1)
        for w in bounce:
            w.start()

    def after():
        for w in bounce:
            w.wait()
        for w in settle:
            w.start()

    todo[steps + 1].append(before)
    todo[steps + 3].append(after)

    def body(t, _):
        c, qb, slot = lax.div(t, steps), lax.rem(t, steps), lax.rem(t, 2)
        for at, jobs in todo.items():
            if jobs:
                @pl.when(t == at)
                def _():
                    for job in jobs:
                        job()

        @pl.when(qb == 0)
        def _():
            project(c)

        attend(c, qb)

        @pl.when(t >= 2)
        def _():
            out_copy(t - 2).wait()

        for h in range(HEADS):
            at = slice(h * BQ, (h + 1) * BQ)
            part = mix_s[:HEAD, at] * (1 / mix_s[HEAD : HEAD + 1, at])
            sout[slot, :, h * HEAD : (h + 1) * HEAD] = part.T.astype(jnp.bfloat16)
        out_copy(t).start()

    lax.fori_loop(0, chunks * steps, body, None)

    for r in range(1 + chunks, rounds):
        s4(r)
    for r in range(rounds):
        if r != 1:
            sent(r)
    for kind in range(6):
        kv_copy(kind).wait_send()
    for w in settle:
        w.wait()
    out_copy(chunks * steps - 2).wait()
    out_copy(chunks * steps - 1).wait()


def solution(mesh):
    def step(x, gain, wq, wk, wv, wo):
        own, d = x.shape
        deep, width = wq.shape
        kvw = wk.shape[1]
        n = d // deep
        chunks, kv_heads = width // COLS, kvw // HEAD
        place = lax.axis_index("sp") * own + jnp.arange(own)
        half = HEAD // 2
        angle = place.astype(jnp.float32)[:, None] * THETA ** (-jnp.arange(half, dtype=jnp.float32) / half)
        cos, sin = jnp.cos(angle), jnp.sin(angle)
        cos, sin = jnp.concatenate([cos, cos], -1), jnp.concatenate([-sin, sin], -1)
        anywhere, vmem = pl.BlockSpec(memory_space=pl.ANY), pl.BlockSpec(memory_space=pltpu.VMEM)
        rounds = 1 + 2 * chunks
        seen, wo = pl.pallas_call(
            functools.partial(_kernel, chunks, kv_heads),
            out_shape=[jax.ShapeDtypeStruct((own, width), jnp.bfloat16), jax.ShapeDtypeStruct((n * deep, d), jnp.bfloat16)],
            in_specs=[vmem] * 3 + [anywhere] * 5,
            out_specs=[anywhere] * 2,
            scratch_shapes=[
                pltpu.VMEM((own, d), jnp.bfloat16),
                pltpu.VMEM((chunks, n * deep, COLS), jnp.bfloat16),
                pltpu.VMEM((n * deep, 2 * kvw), jnp.bfloat16),
                pltpu.VMEM((kv_heads, n * own, HEAD), jnp.bfloat16),
                pltpu.VMEM((kv_heads, DV, n * own), jnp.bfloat16),
                pltpu.VMEM((HEADS, own, HEAD), jnp.bfloat16),
                pltpu.VMEM((2, 128, d), jnp.bfloat16),
                pltpu.VMEM((2, BQ, COLS), jnp.bfloat16),
                pltpu.VMEM((1, HEADS * BQ), jnp.float32),
                pltpu.VMEM((DV, HEADS * BQ), jnp.float32),
                pltpu.SemaphoreType.DMA((rounds, 13)),
                pltpu.SemaphoreType.DMA((rounds, 13)),
                pltpu.SemaphoreType.DMA((6,)),
                pltpu.SemaphoreType.DMA((6,)),
                pltpu.SemaphoreType.DMA((2,)),
                pltpu.SemaphoreType.DMA((2,)),
                pltpu.SemaphoreType.DMA((max(chunks, 2),)),
                pltpu.SemaphoreType.DMA((chunks,)),
                pltpu.SemaphoreType.DMA((chunks,)),
            ],
            compiler_params=pltpu.CompilerParams(collective_id=0, has_side_effects=True, vmem_limit_bytes=VMEM),
        )(cos, sin, gain[None], x, wq, wk, wv, wo)
        y = jnp.dot(seen, wo, preferred_element_type=jnp.float32)
        return (x.astype(jnp.float32) + y).astype(jnp.bfloat16)

    tokens, whole = P(("dp", "sp"), None), P("sp", None)
    return jax.shard_map(
        step,
        mesh=mesh,
        in_specs=(tokens, P(None), whole, whole, whole, whole),
        out_specs=tokens,
        check_vma=False,
    )
```

```python
import functools

import jax
import jax.numpy as jnp
from jax import lax
from jax.experimental import pallas as pl
from jax.experimental.pallas import tpu as pltpu
from jax.sharding import PartitionSpec as P

HEAD = 128
THETA = 10000
NEG = -1e30
HIDDEN = 2 * NEG
LOG2E = 1.4426950408889634
VMEM = 67043328
MESH = pl.DeviceIdType.MESH

HEADS = 8
COLS = HEADS * HEAD
BQ = 256
BK = 512
STRIP = 512
DV = HEAD + 16

XRA, XLA, XRB, XLB, RR, RL, Q1A, Q2A, Q1B, Q2B, Q3A, Q3B, D1, D2, D3, D4, D5, D6 = range(18)
KR, KL, VR, VL, KRR, VLL = range(6)
LIGHT = (0, 1, 5)


def _dot(a, b, ca, cb):
    return lax.dot_general(a, b, (((ca,), (cb,)), ((), ())), preferred_element_type=jnp.float32)


def _kernel(chunks, kv_heads, cos_ref, sin_ref, gain_ref, x_ref, wq_ref, wk_ref, wv_ref, wo_ref, seen_ref, wof_ref,
            a_s, wq_s, k_s, v_s, q_s, xin, sout, top_s, mix_s, s_s, ss, rs, kss, krs, xsem, osem, lsem, wsem, bsem):
    own = x_ref.shape[0]
    deep = wq_ref.shape[0]
    dp, me = lax.axis_index("dp"), lax.axis_index("sp")
    n = lax.axis_size("sp")
    right, left, far = lax.rem(me + 1, n), lax.rem(me + n - 1, n), lax.rem(me + 2, n)
    core = lax.rem(dp, 2)
    p = lax.rem(lax.div(dp, 2), 2)
    mate = {"dp": dp + 1 - 2 * core, "sp": me}
    pair = {"dp": dp + 2 - 4 * p, "sp": me}
    to_right, to_left = {"dp": dp, "sp": right}, {"dp": dp, "sp": left}
    half, quarter = deep // 2, deep // 8

    barrier = pltpu.get_barrier_semaphore()
    for other in (mate, pair, to_right, to_left):
        pl.semaphore_signal(barrier, inc=1, device_id=other, device_id_type=MESH)
    pl.semaphore_wait(barrier, 4)

    kvw = wk_ref.shape[1]
    rounds = 1 + 2 * chunks

    def place(r, shard, row, size):
        at = pl.ds(pl.multiple_of(shard * deep + row, 128), size)
        if r == 0:
            return wq_s.at[chunks - 1, at, pl.ds(0, 2 * kvw)]
        if r <= chunks:
            return wq_s.at[r - 1, at, :]
        return wof_ref.at[at, pl.ds((r - 1 - chunks) * COLS, COLS)]

    def source(r, row, size):
        if r == 0:
            return place(r, me, row, size)
        at = pl.ds(pl.multiple_of(row, 128), size)
        c = (r - 1) % chunks
        return (wq_ref if r <= chunks else wo_ref).at[at, pl.ds(c * COLS, COLS)]

    def kinds_of(r):
        return [kind for kind in range(18) if r in LIGHT or kind not in (Q1B, Q2B)]

    def copy(r, kind, arriving=False):
        b, pp = core * half, p
        if arriving and kind in (Q1A, Q2A, Q1B, Q2B, Q3A, Q3B):
            pp = 1 - p
        if arriving and kind >= D1:
            b = (1 - core) * half
        light = r in LIGHT
        edge, inner = (3 * pp, 1), (1 + pp, 1)
        mine, others = (2 * pp, 2), (2 * (1 - pp), 2)
        (first, size), shard, to = {
            XRA: (edge, left if arriving else me, to_right),
            XLA: (edge, right if arriving else me, to_left),
            XRB: (inner if light else (1, 2), left if arriving else me, to_right),
            XLB: (inner if light else (1, 2), right if arriving else me, to_left),
            RR: (inner, far if arriving else left, to_right),
            RL: (edge, far if arriving else right, to_left),
            Q1A: (edge, left, pair),
            Q2A: (edge, right, pair),
            Q1B: (inner, left, pair),
            Q2B: (inner, right, pair),
            Q3A: (inner, far, pair),
            Q3B: (edge, far, pair),
            D1: (mine if light else (pp, 3), left, mate),
            D2: (mine if light else (pp, 3), right, mate),
            D3: (others if light else (3 * (1 - pp), 1), left, mate),
            D4: (others if light else (3 * (1 - pp), 1), right, mate),
            D5: (mine, far, mate),
            D6: (others, far, mate),
        }[kind]
        row, size = b + first * quarter, size * quarter
        dst = place(r, shard, row, size)
        src = source(r, row, size) if kind <= XLB and not arriving else dst
        return pltpu.make_async_remote_copy(src_ref=src, dst_ref=dst, send_sem=ss.at[r, kind], recv_sem=rs.at[r, kind],
                                            device_id=to, device_id_type=MESH)

    def start(r, *kinds):
        for kind in kinds:
            if kind in kinds_of(r):
                copy(r, kind).start()

    def arrive(r, *kinds):
        for kind in kinds:
            if kind in kinds_of(r):
                copy(r, kind, True).wait_recv()

    def sent(r):
        for kind in kinds_of(r):
            copy(r, kind).wait_send()

    def s0a(r):
        start(r, XRA, XLA)

    def s0b(r):
        start(r, XRB, XLB)

    def s0(r):
        s0a(r)
        s0b(r)

    def s1a(r):
        arrive(r, XRA)
        start(r, Q1A)
        arrive(r, XLA)
        start(r, Q2A, RL)

    def s1b(r):
        arrive(r, XRB)
        start(r, RR, Q1B, D1)
        arrive(r, XLB)
        start(r, Q2B, D2)

    def s2(r):
        arrive(r, RL)
        start(r, Q3B)
        arrive(r, RR)
        start(r, Q3A, D5)
        arrive(r, Q1A, Q2A, Q1B, Q2B)
        start(r, D3, D4)

    def s3(r):
        arrive(r, Q3A, Q3B)
        start(r, D6)

    def s4(r):
        arrive(r, D1, D2, D3, D4, D5, D6)

    def kv_copy(kind, arriving=False):
        shard = {KR: left if arriving else me, KL: right if arriving else me, VR: left if arriving else me,
                 VL: right if arriving else me, KRR: far if arriving else left, VLL: far if arriving else right}[kind]
        to = to_right if kind in (KR, VR, KRR) else to_left
        at = pl.ds(pl.multiple_of(shard * own, 128), own)
        ref = k_s.at[:, at, :] if kind in (KR, KL, KRR) else v_s.at[:, pl.ds(0, HEAD), at]
        return pltpu.make_async_remote_copy(src_ref=ref, dst_ref=ref, send_sem=kss.at[kind], recv_sem=krs.at[kind],
                                            device_id=to, device_id_type=MESH)

    mine = pl.ds(pl.multiple_of(me * deep, 128), deep)
    wk_in = pltpu.make_async_copy(wk_ref, wq_s.at[chunks - 1, mine, pl.ds(0, kvw)], lsem.at[0])
    wv_in = pltpu.make_async_copy(wv_ref, wq_s.at[chunks - 1, mine, pl.ds(kvw, kvw)], lsem.at[1])
    wk_in.start()
    wv_in.start()
    rows = xin.shape[1]
    x_in = [pltpu.make_async_copy(x_ref.at[pl.ds(i * rows, rows), :], xin.at[i % 2], xsem.at[i % 2]) for i in range(own // rows)]
    x_in[0].start()
    x_in[1].start()
    wk_in.wait()
    wv_in.wait()
    s0(0)
    wq_in = [pltpu.make_async_copy(wq_ref.at[:, pl.ds(c * COLS, COLS)], wq_s.at[c, mine, :], wsem.at[c]) for c in range(chunks)]
    for w in wq_in[:-1]:
        w.start()

    for i, block in enumerate(x_in):
        block.wait()
        wide = xin[i % 2].astype(jnp.float32)
        scale = lax.rsqrt(jnp.mean(wide * wide, -1, keepdims=True) + 1e-6)
        a_s[i * rows : (i + 1) * rows, :] = (wide * scale * gain_ref[...].astype(jnp.float32)).astype(jnp.bfloat16)
        if i + 2 < len(x_in):
            x_in[i + 2].start()
        if i == len(x_in) // 2:
            s1a(0)
    for h in range(kv_heads):
        v_s[h, HEAD:, :] = jnp.ones((DV - HEAD, v_s.shape[2]), jnp.bfloat16)

    s1b(0)
    s0(1)
    s2(0)
    s3(0)
    s1a(1)
    s4(0)

    def turn(t, at):
        wide = t.astype(jnp.bfloat16).astype(jnp.float32)
        return (wide * cos_ref[at, :] + pltpu.roll(wide, HEAD // 2, 1) * sin_ref[at, :]).astype(jnp.bfloat16)

    def keys_values(i, _):
        at = pl.ds(pl.multiple_of(i * BQ, BQ), BQ)
        there = pl.ds(pl.multiple_of(me * own + i * BQ, BQ), BQ)
        kv = _dot(a_s[at, :], wq_s[chunks - 1, :, : 2 * kvw], 1, 0)
        for h in range(kv_heads):
            k_s[h, there, :] = turn(kv[:, h * HEAD : (h + 1) * HEAD], at)
            v_s[h, :HEAD, there] = kv[:, kvw + h * HEAD : kvw + (h + 1) * HEAD].astype(jnp.bfloat16).T
        return _

    lax.fori_loop(0, own // BQ, keys_values, None)
    sent(0)
    wq_in[-1].start()

    s1b(1)
    for kind in (KR, VL, VR, KL):
        kv_copy(kind).start()
    s2(1)
    s3(1)
    s4(1)
    wq_in[0].wait()

    group = 2
    tall = own // 2

    def project(c):
        def tile(i, _):
            m, j = lax.div(i, HEADS // group), lax.rem(i, HEADS // group)
            at = pl.ds(pl.multiple_of(m * tall, tall), tall)
            cols = pl.ds(pl.multiple_of(j * group * HEAD, group * HEAD), group * HEAD)
            q = _dot(a_s[at, :], wq_s[c, :, cols], 1, 0)
            for h in range(group):
                q_s[j * group + h, at, :] = turn(q[:, h * HEAD : (h + 1) * HEAD], at)
            return _

        lax.fori_loop(0, 2 * (HEADS // group), tile, None)

    e = HEAD**-0.5 * LOG2E
    wide = HEADS * BQ
    strips = list(range(0, wide, STRIP))

    def attend(c, qb):
        g = lax.div(c * kv_heads, chunks)
        first = me * own + qb * BQ
        q = q_s[:, pl.ds(pl.multiple_of(qb * BQ, BQ), BQ), :].reshape(wide, HEAD)
        top_s[...] = jnp.full(top_s.shape, NEG, jnp.float32)
        mix_s[...] = jnp.zeros(mix_s.shape, jnp.float32)

        def scores(j, at):
            s_s[:, at : at + STRIP] = _dot(k_s[g, pl.ds(pl.multiple_of(j * BK, BK), BK), :], q[at : at + STRIP], 1, 1)

        def block(j, last):
            values = v_s[g, :, pl.ds(pl.multiple_of(j * BK, BK), BK)]
            if last:
                gap = lax.rem(lax.broadcasted_iota(jnp.int32, (BK, STRIP), 1), BQ) - lax.broadcasted_iota(jnp.int32, (BK, STRIP), 0)
                ok = gap >= j * BK - first
            for at in strips:
                s = s_s[:, at : at + STRIP]
                if last:
                    s = jnp.where(ok, s, HIDDEN)
                old = top_s[:, at : at + STRIP]
                top = jnp.maximum(old, s.max(axis=0, keepdims=True))
                top_s[:, at : at + STRIP] = top
                w, keep = jnp.exp2((s - top) * e).astype(jnp.bfloat16), jnp.exp2((old - top) * e)
                if not last:
                    scores(j + 1, at)
                mix_s[:, at : at + STRIP] = mix_s[:, at : at + STRIP] * keep + _dot(values, w, 1, 0)

        whole = lax.div(first + 1, BK)
        for at in strips:
            scores(0, at)
        lax.fori_loop(0, whole, lambda j, _: block(j, False), None)
        block(whole, True)

    steps = own // BQ

    def out_copy(t):
        c, qb, slot = lax.div(t, steps), lax.rem(t, steps), lax.rem(t, 2)
        return pltpu.make_async_copy(sout.at[slot], seen_ref.at[pl.ds(pl.multiple_of(qb * BQ, BQ), BQ), pl.ds(pl.multiple_of(c * COLS, COLS), COLS)],
                                     osem.at[slot])

    bounce = [pltpu.make_async_copy(wo_ref.at[:, pl.ds(c * COLS, COLS)], wq_s.at[0, pl.ds(c * deep, deep), :], bsem.at[c]) for c in range(chunks)]
    settle = [pltpu.make_async_copy(wq_s.at[0, pl.ds(c * deep, deep), :], wof_ref.at[mine, pl.ds(c * COLS, COLS)], lsem.at[c])
              for c in range(chunks)]

    todo = {t: [] for t in range(chunks * steps + 1)}
    for i, r in enumerate(range(2, rounds)):
        todo[2 * i + 1].append(functools.partial(s1a, r))
        todo[2 * i + 2].append(functools.partial(s1b, r))
        if r == 2:
            todo[2].append(functools.partial(s0b, 3))
        if r + 2 < rounds:
            todo[2 * i + 2].append(functools.partial(s0, r + 2))
        todo[2 * i + 3].append(functools.partial(s2, r))
        todo[2 * i + 4].append(functools.partial(s3, r))
    for c in range(1, chunks):
        todo[steps * c] += [functools.partial(s4, 1 + c), wq_in[c].wait]

    def before():
        sent(1)
        for w in bounce:
            w.start()

    def after():
        for w in bounce:
            w.wait()
        for w in settle:
            w.start()

    todo[steps + 1].append(before)
    todo[steps + 3].append(after)

    def body(t, _):
        c, qb, slot = lax.div(t, steps), lax.rem(t, steps), lax.rem(t, 2)
        for at, jobs in todo.items():
            if jobs and at < chunks * steps:
                @pl.when(t == at)
                def _():
                    for job in jobs:
                        job()

        @pl.when((qb == 0) & (c > 0))
        def _():
            project(c)

        attend(c, qb)

        @pl.when(t >= 2)
        def _():
            out_copy(t - 2).wait()

        for h in range(HEADS):
            at = slice(h * BQ, (h + 1) * BQ)
            part = mix_s[:HEAD, at] * (1 / mix_s[HEAD : HEAD + 1, at])
            sout[slot, :, h * HEAD : (h + 1) * HEAD] = part.T.astype(jnp.bfloat16)
        out_copy(t).start()

    kv_copy(KR, True).wait_recv()
    kv_copy(KRR).start()
    kv_copy(VL, True).wait_recv()
    kv_copy(VLL).start()
    s0(2)
    s0a(3)
    project(0)
    for kind in (KL, VR, KRR, VLL):
        kv_copy(kind, True).wait_recv()
    lax.fori_loop(0, chunks * steps, body, None)

    for job in todo[chunks * steps]:
        job()
    for r in range(1 + chunks, rounds):
        s4(r)
    for r in range(2, rounds):
        sent(r)
    for kind in range(6):
        kv_copy(kind).wait_send()
    for w in settle:
        w.wait()
    out_copy(chunks * steps - 2).wait()
    out_copy(chunks * steps - 1).wait()


def solution(mesh):
    def step(x, gain, wq, wk, wv, wo):
        own, d = x.shape
        deep, width = wq.shape
        kvw = wk.shape[1]
        n = d // deep
        chunks, kv_heads = width // COLS, kvw // HEAD
        place = lax.axis_index("sp") * own + jnp.arange(own)
        half = HEAD // 2
        angle = place.astype(jnp.float32)[:, None] * THETA ** (-jnp.arange(half, dtype=jnp.float32) / half)
        cos, sin = jnp.cos(angle), jnp.sin(angle)
        cos, sin = jnp.concatenate([cos, cos], -1), jnp.concatenate([-sin, sin], -1)
        anywhere, vmem = pl.BlockSpec(memory_space=pl.ANY), pl.BlockSpec(memory_space=pltpu.VMEM)
        rounds = 1 + 2 * chunks
        seen, wo = pl.pallas_call(
            functools.partial(_kernel, chunks, kv_heads),
            out_shape=[jax.ShapeDtypeStruct((own, width), jnp.bfloat16), jax.ShapeDtypeStruct((n * deep, d), jnp.bfloat16)],
            in_specs=[vmem] * 3 + [anywhere] * 5,
            out_specs=[anywhere] * 2,
            scratch_shapes=[
                pltpu.VMEM((own, d), jnp.bfloat16),
                pltpu.VMEM((chunks, n * deep, COLS), jnp.bfloat16),
                pltpu.VMEM((kv_heads, n * own, HEAD), jnp.bfloat16),
                pltpu.VMEM((kv_heads, DV, n * own), jnp.bfloat16),
                pltpu.VMEM((HEADS, own, HEAD), jnp.bfloat16),
                pltpu.VMEM((2, 128, d), jnp.bfloat16),
                pltpu.VMEM((2, BQ, COLS), jnp.bfloat16),
                pltpu.VMEM((1, HEADS * BQ), jnp.float32),
                pltpu.VMEM((DV, HEADS * BQ), jnp.float32),
                pltpu.VMEM((BK, HEADS * BQ), jnp.float32),
                pltpu.SemaphoreType.DMA((rounds, 18)),
                pltpu.SemaphoreType.DMA((rounds, 18)),
                pltpu.SemaphoreType.DMA((6,)),
                pltpu.SemaphoreType.DMA((6,)),
                pltpu.SemaphoreType.DMA((2,)),
                pltpu.SemaphoreType.DMA((2,)),
                pltpu.SemaphoreType.DMA((max(chunks, 2),)),
                pltpu.SemaphoreType.DMA((chunks,)),
                pltpu.SemaphoreType.DMA((chunks,)),
            ],
            compiler_params=pltpu.CompilerParams(collective_id=0, has_side_effects=True, vmem_limit_bytes=VMEM),
        )(cos, sin, gain[None], x, wq, wk, wv, wo)
        y = jnp.dot(seen, wo, preferred_element_type=jnp.float32)
        return (x.astype(jnp.float32) + y).astype(jnp.bfloat16)

    tokens, whole = P(("dp", "sp"), None), P("sp", None)
    return jax.shard_map(
        step,
        mesh=mesh,
        in_specs=(tokens, P(None), whole, whole, whole, whole),
        out_specs=tokens,
        check_vma=False,
    )
```

```python
import functools

import jax
import jax.numpy as jnp
from jax import lax
from jax.experimental import pallas as pl
from jax.experimental.pallas import tpu as pltpu
from jax.sharding import PartitionSpec as P

HEAD = 128
THETA = 10000
NEG = -1e30
HIDDEN = 2 * NEG
LOG2E = 1.4426950408889634
VMEM = 67043328
MESH = pl.DeviceIdType.MESH

HEADS = 8
COLS = HEADS * HEAD
BQ = 256
BK = 512
STRIP = 512
DV = HEAD + 16

XRA, XLA, XRB, XLB, RR, RL, Q1A, Q2A, Q1B, Q2B, Q3A, Q3B, D1, D2, D3, D4, D5, D6 = range(18)
KR, KL, VR, VL, KRR, VLL = range(6)
S0A, S0B, S1A, S1B, S2, S3 = range(6)
PLAN = ((1, 0, S1A, 2), (2, 0, S1B, 2), (2, 0, S0B, 3), (2, 0, S0A, 4), (2, 0, S0B, 4), (2, 2, S2, 2), (3, 2, S1A, 3), (3, 2, S3, 2),
        (4, 0, S1B, 3), (4, 0, S0A, 5), (4, 1, S1A, 4), (4, 1, S0A, 6), (4, 2, S2, 3), (4, 2, S0A, 7), (5, 0, S1B, 4), (6, 0, S0A, 8),
        (6, 0, S1A, 5), (6, 2, S3, 3), (7, 0, S0B, 5), (7, 2, S0B, 8), (7, 2, S2, 4), (8, 0, S1A, 7), (8, 0, S1A, 8), (9, 0, S1B, 5),
        (9, 2, S0B, 7), (9, 2, S0B, 6), (10, 0, S3, 4), (10, 0, S1A, 6), (11, 2, S2, 5), (12, 0, S1B, 8), (12, 1, S2, 8),
        (12, 1, S1B, 7), (12, 2, S1B, 6), (13, 0, S2, 7), (13, 2, S2, 6), (14, 2, S3, 5), (15, 0, S3, 7), (15, 0, S3, 8), (16, 0, S3, 6))
LIGHT = (1,)


def _dot(a, b, ca, cb):
    return lax.dot_general(a, b, (((ca,), (cb,)), ((), ())), preferred_element_type=jnp.float32)


def _kernel(chunks, kv_heads, cos_ref, sin_ref, gain_ref, x_ref, wq_ref, wk_ref, wv_ref, wo_ref, seen_ref, wof_ref,
            a_s, wq_s, k_s, v_s, q_s, xin, sout, top_s, mix_s, s_s, ss, rs, kss, krs, xsem, osem, lsem, wsem, bsem):
    own = x_ref.shape[0]
    deep = wq_ref.shape[0]
    dp, me = lax.axis_index("dp"), lax.axis_index("sp")
    n = lax.axis_size("sp")
    right, left, far = lax.rem(me + 1, n), lax.rem(me + n - 1, n), lax.rem(me + 2, n)
    core = lax.rem(dp, 2)
    p = lax.rem(lax.div(dp, 2), 2)
    mate = {"dp": dp + 1 - 2 * core, "sp": me}
    pair = {"dp": dp + 2 - 4 * p, "sp": me}
    to_right, to_left = {"dp": dp, "sp": right}, {"dp": dp, "sp": left}
    half, quarter = deep // 2, deep // 8

    barrier = pltpu.get_barrier_semaphore()
    for other in (mate, pair, to_right, to_left):
        pl.semaphore_signal(barrier, inc=1, device_id=other, device_id_type=MESH)
    pl.semaphore_wait(barrier, 4)

    kvw = wk_ref.shape[1]
    rounds = 1 + 2 * chunks

    def place(r, shard, row, size):
        at = pl.ds(pl.multiple_of(shard * deep + row, 128), size)
        if r == 0:
            return wq_s.at[chunks - 1, at, pl.ds(0, 2 * kvw)]
        if r <= chunks:
            return wq_s.at[r - 1, at, :]
        return wof_ref.at[at, pl.ds((r - 1 - chunks) * COLS, COLS)]

    def source(r, row, size):
        if r == 0:
            return place(r, me, row, size)
        at = pl.ds(pl.multiple_of(row, 128), size)
        c = (r - 1) % chunks
        return (wq_ref if r <= chunks else wo_ref).at[at, pl.ds(c * COLS, COLS)]

    def kinds_of(r):
        return [kind for kind in range(18) if r in LIGHT or kind not in (Q1B, Q2B)]

    def copy(r, kind, arriving=False):
        b, pp = core * half, p
        if arriving and kind in (Q1A, Q2A, Q1B, Q2B, Q3A, Q3B):
            pp = 1 - p
        if arriving and kind >= D1:
            b = (1 - core) * half
        light = r in LIGHT
        edge, inner = (3 * pp, 1), (1 + pp, 1)
        mine, others = (2 * pp, 2), (2 * (1 - pp), 2)
        (first, size), shard, to = {
            XRA: (edge, left if arriving else me, to_right),
            XLA: (edge, right if arriving else me, to_left),
            XRB: (inner if light else (1, 2), left if arriving else me, to_right),
            XLB: (inner if light else (1, 2), right if arriving else me, to_left),
            RR: (inner, far if arriving else left, to_right),
            RL: (edge, far if arriving else right, to_left),
            Q1A: (edge, left, pair),
            Q2A: (edge, right, pair),
            Q1B: (inner, left, pair),
            Q2B: (inner, right, pair),
            Q3A: (inner, far, pair),
            Q3B: (edge, far, pair),
            D1: (mine if light else (pp, 3), left, mate),
            D2: (mine if light else (pp, 3), right, mate),
            D3: (others if light else (3 * (1 - pp), 1), left, mate),
            D4: (others if light else (3 * (1 - pp), 1), right, mate),
            D5: (mine, far, mate),
            D6: (others, far, mate),
        }[kind]
        row, size = b + first * quarter, size * quarter
        dst = place(r, shard, row, size)
        src = source(r, row, size) if kind <= XLB and not arriving else dst
        return pltpu.make_async_remote_copy(src_ref=src, dst_ref=dst, send_sem=ss.at[r, kind], recv_sem=rs.at[r, kind],
                                            device_id=to, device_id_type=MESH)

    def start(r, *kinds):
        for kind in kinds:
            if kind in kinds_of(r):
                copy(r, kind).start()

    def arrive(r, *kinds):
        for kind in kinds:
            if kind in kinds_of(r):
                copy(r, kind, True).wait_recv()

    def sent(r):
        for kind in kinds_of(r):
            copy(r, kind).wait_send()

    def s0a(r):
        start(r, XRA, XLA)

    def s0b(r):
        start(r, XRB, XLB)

    def s0(r):
        s0a(r)
        s0b(r)

    def s1a(r):
        arrive(r, XRA)
        start(r, Q1A)
        arrive(r, XLA)
        start(r, Q2A, RL)

    def s1b(r):
        arrive(r, XRB)
        start(r, RR, Q1B, D1)
        arrive(r, XLB)
        start(r, Q2B, D2)

    def s2(r):
        arrive(r, RL)
        start(r, Q3B)
        arrive(r, RR)
        start(r, Q3A, D5)
        arrive(r, Q1A, Q2A, Q1B, Q2B)
        start(r, D3, D4)

    def s3(r):
        arrive(r, Q3A, Q3B)
        start(r, D6)

    def s4(r):
        arrive(r, D1, D2, D3, D4, D5, D6)

    def kv_copy(kind, arriving=False):
        shard = {KR: left if arriving else me, KL: right if arriving else me, VR: left if arriving else me,
                 VL: right if arriving else me, KRR: far if arriving else left, VLL: far if arriving else right}[kind]
        to = to_right if kind in (KR, VR, KRR) else to_left
        at = pl.ds(pl.multiple_of(shard * own, 128), own)
        ref = k_s.at[:, at, :] if kind in (KR, KL, KRR) else v_s.at[:, pl.ds(0, HEAD), at]
        return pltpu.make_async_remote_copy(src_ref=ref, dst_ref=ref, send_sem=kss.at[kind], recv_sem=krs.at[kind],
                                            device_id=to, device_id_type=MESH)

    mine = pl.ds(pl.multiple_of(me * deep, 128), deep)
    wk_in = pltpu.make_async_copy(wk_ref, wq_s.at[chunks - 1, mine, pl.ds(0, kvw)], lsem.at[0])
    wv_in = pltpu.make_async_copy(wv_ref, wq_s.at[chunks - 1, mine, pl.ds(kvw, kvw)], lsem.at[1])
    wk_in.start()
    wv_in.start()
    rows = xin.shape[1]
    x_in = [pltpu.make_async_copy(x_ref.at[pl.ds(i * rows, rows), :], xin.at[i % 2], xsem.at[i % 2]) for i in range(own // rows)]
    x_in[0].start()
    x_in[1].start()
    wk_in.wait()
    wv_in.wait()
    s0(0)
    wq_in = [pltpu.make_async_copy(wq_ref.at[:, pl.ds(c * COLS, COLS)], wq_s.at[c, mine, :], wsem.at[c]) for c in range(chunks)]
    for w in wq_in[:-1]:
        w.start()

    for i, block in enumerate(x_in):
        block.wait()
        wide = xin[i % 2].astype(jnp.float32)
        scale = lax.rsqrt(jnp.mean(wide * wide, -1, keepdims=True) + 1e-6)
        a_s[i * rows : (i + 1) * rows, :] = (wide * scale * gain_ref[...].astype(jnp.float32)).astype(jnp.bfloat16)
        if i + 2 < len(x_in):
            x_in[i + 2].start()
        if i == len(x_in) // 2:
            s1a(0)
    for h in range(kv_heads):
        v_s[h, HEAD:, :] = jnp.ones((DV - HEAD, v_s.shape[2]), jnp.bfloat16)

    s1b(0)
    s0(1)
    s2(0)
    s3(0)
    s1a(1)
    s4(0)
    s1b(1)

    def turn(t, at):
        wide = t.astype(jnp.bfloat16).astype(jnp.float32)
        return (wide * cos_ref[at, :] + pltpu.roll(wide, HEAD // 2, 1) * sin_ref[at, :]).astype(jnp.bfloat16)

    def keys_values(i, _):
        at = pl.ds(pl.multiple_of(i * BQ, BQ), BQ)
        there = pl.ds(pl.multiple_of(me * own + i * BQ, BQ), BQ)
        kv = _dot(a_s[at, :], wq_s[chunks - 1, :, : 2 * kvw], 1, 0)
        for h in range(kv_heads):
            k_s[h, there, :] = turn(kv[:, h * HEAD : (h + 1) * HEAD], at)
            v_s[h, :HEAD, there] = kv[:, kvw + h * HEAD : kvw + (h + 1) * HEAD].astype(jnp.bfloat16).T
        return _

    lax.fori_loop(0, own // BQ, keys_values, None)
    sent(0)
    wq_in[-1].start()

    for kind in (KR, VL, VR, KL):
        kv_copy(kind).start()
    s2(1)
    s3(1)
    s4(1)
    wq_in[0].wait()

    group = 2
    tall = own // 2

    def project(c):
        def tile(i, _):
            m, j = lax.div(i, HEADS // group), lax.rem(i, HEADS // group)
            at = pl.ds(pl.multiple_of(m * tall, tall), tall)
            cols = pl.ds(pl.multiple_of(j * group * HEAD, group * HEAD), group * HEAD)
            q = _dot(a_s[at, :], wq_s[c, :, cols], 1, 0)
            for h in range(group):
                q_s[j * group + h, at, :] = turn(q[:, h * HEAD : (h + 1) * HEAD], at)
            return _

        lax.fori_loop(0, 2 * (HEADS // group), tile, None)

    e = HEAD**-0.5 * LOG2E
    wide = HEADS * BQ
    strips = list(range(0, wide, STRIP))

    def attend(c, qb, between):
        g = lax.div(c * kv_heads, chunks)
        first = me * own + qb * BQ

        def queries(i):
            return q_s[:, pl.ds(pl.multiple_of(i * BQ, BQ), BQ), :].reshape(wide, HEAD)

        q = queries(qb)
        top_s[...] = jnp.full(top_s.shape, NEG, jnp.float32)
        mix_s[...] = jnp.zeros(mix_s.shape, jnp.float32)

        def scores(j, at, q):
            s_s[:, at : at + STRIP] = _dot(k_s[g, pl.ds(pl.multiple_of(j * BK, BK), BK), :], q[at : at + STRIP], 1, 1)

        def block(j, size, last):
            values = v_s[g, :, pl.ds(pl.multiple_of(j * BK, BK), size)]
            if last:
                gap = lax.rem(lax.broadcasted_iota(jnp.int32, (size, STRIP), 1), BQ) - lax.broadcasted_iota(jnp.int32, (size, STRIP), 0)
                ok = gap >= j * BK - first
            for at in strips:
                s = s_s[:size, at : at + STRIP]
                if last:
                    s = jnp.where(ok, s, HIDDEN)
                old = top_s[:, at : at + STRIP]
                top = jnp.maximum(old, s.max(axis=0, keepdims=True))
                top_s[:, at : at + STRIP] = top
                w, keep = jnp.exp2((s - top) * e).astype(jnp.bfloat16), jnp.exp2((old - top) * e)
                if last:
                    scores(0, at, later)
                else:
                    scores(j + 1, at, q)
                mix_s[:, at : at + STRIP] = mix_s[:, at : at + STRIP] * keep + _dot(values, w, 1, 0)

        whole = lax.div(first + 1, BK)
        later = queries(lax.rem(qb + 1, own // BQ))

        @pl.when(qb == 0)
        def _():
            for at in strips:
                scores(0, at, q)

        lax.fori_loop(0, whole, lambda j, _: block(j, BK, False), None)
        between()

        @pl.when(lax.rem(qb, 2) == 0)
        def _():
            block(whole, BQ, True)

        @pl.when(lax.rem(qb, 2) == 1)
        def _():
            block(whole, BK, True)

    steps = own // BQ

    def out_copy(t):
        c, qb, slot = lax.div(t, steps), lax.rem(t, steps), lax.rem(t, 2)
        return pltpu.make_async_copy(sout.at[slot], seen_ref.at[pl.ds(pl.multiple_of(qb * BQ, BQ), BQ), pl.ds(pl.multiple_of(c * COLS, COLS), COLS)],
                                     osem.at[slot])

    bounce = [pltpu.make_async_copy(wo_ref.at[:, pl.ds(c * COLS, COLS)], wq_s.at[0, pl.ds(c * deep, deep), :], bsem.at[c]) for c in range(chunks)]
    settle = [pltpu.make_async_copy(wq_s.at[0, pl.ds(c * deep, deep), :], wof_ref.at[mine, pl.ds(c * COLS, COLS)], lsem.at[c])
              for c in range(chunks)]

    end = chunks * steps
    todo = {}
    for t, part, stage, r in PLAN:
        todo.setdefault((t, part), []).append(functools.partial((s0a, s0b, s1a, s1b, s2, s3)[stage], r))
    for c in range(1, chunks):
        todo.setdefault((steps * c, 0), []).extend([functools.partial(s4, 1 + c), wq_in[c].wait])

    def before():
        sent(1)
        for w in bounce:
            w.start()

    def after():
        for w in bounce:
            w.wait()
        for w in settle:
            w.start()

    todo.setdefault((steps + 1, 0), []).append(before)
    todo.setdefault((steps + 3, 0), []).append(after)

    def links(t, part):
        for (at, where), jobs in todo.items():
            if where == part and at < end:
                @pl.when(t == at)
                def _():
                    for job in jobs:
                        job()

    def body(t, _):
        c, qb, slot = lax.div(t, steps), lax.rem(t, steps), lax.rem(t, 2)
        links(t, 0)

        @pl.when((qb == 0) & (c > 0))
        def _():
            project(c)

        links(t, 1)
        attend(c, qb, functools.partial(links, t, 2))

        @pl.when(t >= 2)
        def _():
            out_copy(t - 2).wait()

        for h in range(HEADS):
            at = slice(h * BQ, (h + 1) * BQ)
            part = mix_s[:HEAD, at] * (1 / mix_s[HEAD : HEAD + 1, at])
            sout[slot, :, h * HEAD : (h + 1) * HEAD] = part.T.astype(jnp.bfloat16)
        out_copy(t).start()

    kv_copy(KR, True).wait_recv()
    kv_copy(KRR).start()
    kv_copy(VL, True).wait_recv()
    kv_copy(VLL).start()
    s0(2)
    s0a(3)
    project(0)
    for kind in (KL, VR, KRR, VLL):
        kv_copy(kind, True).wait_recv()
    lax.fori_loop(0, chunks * steps, body, None)

    for job in todo.get((end, 0), []):
        job()
    for r in range(1 + chunks, rounds):
        s4(r)
    for r in range(2, rounds):
        sent(r)
    for kind in range(6):
        kv_copy(kind).wait_send()
    for w in settle:
        w.wait()
    out_copy(chunks * steps - 2).wait()
    out_copy(chunks * steps - 1).wait()


def solution(mesh):
    def step(x, gain, wq, wk, wv, wo):
        own, d = x.shape
        deep, width = wq.shape
        kvw = wk.shape[1]
        n = d // deep
        chunks, kv_heads = width // COLS, kvw // HEAD
        place = lax.axis_index("sp") * own + jnp.arange(own)
        half = HEAD // 2
        angle = place.astype(jnp.float32)[:, None] * THETA ** (-jnp.arange(half, dtype=jnp.float32) / half)
        cos, sin = jnp.cos(angle), jnp.sin(angle)
        cos, sin = jnp.concatenate([cos, cos], -1), jnp.concatenate([-sin, sin], -1)
        anywhere, vmem = pl.BlockSpec(memory_space=pl.ANY), pl.BlockSpec(memory_space=pltpu.VMEM)
        rounds = 1 + 2 * chunks
        seen, wo = pl.pallas_call(
            functools.partial(_kernel, chunks, kv_heads),
            out_shape=[jax.ShapeDtypeStruct((own, width), jnp.bfloat16), jax.ShapeDtypeStruct((n * deep, d), jnp.bfloat16)],
            in_specs=[vmem] * 3 + [anywhere] * 5,
            out_specs=[anywhere] * 2,
            scratch_shapes=[
                pltpu.VMEM((own, d), jnp.bfloat16),
                pltpu.VMEM((chunks, n * deep, COLS), jnp.bfloat16),
                pltpu.VMEM((kv_heads, n * own, HEAD), jnp.bfloat16),
                pltpu.VMEM((kv_heads, DV, n * own), jnp.bfloat16),
                pltpu.VMEM((HEADS, own, HEAD), jnp.bfloat16),
                pltpu.VMEM((2, 128, d), jnp.bfloat16),
                pltpu.VMEM((2, BQ, COLS), jnp.bfloat16),
                pltpu.VMEM((1, HEADS * BQ), jnp.float32),
                pltpu.VMEM((DV, HEADS * BQ), jnp.float32),
                pltpu.VMEM((BK, HEADS * BQ), jnp.float32),
                pltpu.SemaphoreType.DMA((rounds, 18)),
                pltpu.SemaphoreType.DMA((rounds, 18)),
                pltpu.SemaphoreType.DMA((6,)),
                pltpu.SemaphoreType.DMA((6,)),
                pltpu.SemaphoreType.DMA((2,)),
                pltpu.SemaphoreType.DMA((2,)),
                pltpu.SemaphoreType.DMA((max(chunks, 2),)),
                pltpu.SemaphoreType.DMA((chunks,)),
                pltpu.SemaphoreType.DMA((chunks,)),
            ],
            compiler_params=pltpu.CompilerParams(collective_id=0, has_side_effects=True, vmem_limit_bytes=VMEM),
        )(cos, sin, gain[None], x, wq, wk, wv, wo)
        y = jnp.dot(seen, wo, preferred_element_type=jnp.float32)
        return (x.astype(jnp.float32) + y).astype(jnp.bfloat16)

    tokens, whole = P(("dp", "sp"), None), P("sp", None)
    return jax.shard_map(
        step,
        mesh=mesh,
        in_specs=(tokens, P(None), whole, whole, whole, whole),
        out_specs=tokens,
        check_vma=False,
    )
```

```python
import functools

import jax
import jax.numpy as jnp
from jax import lax
from jax.experimental import pallas as pl
from jax.experimental.pallas import tpu as pltpu
from jax.sharding import PartitionSpec as P

HEAD = 128
THETA = 10000
NEG = -1e30
HIDDEN = 2 * NEG
LOG2E = 1.4426950408889634
VMEM = 67043328
MESH = pl.DeviceIdType.MESH

HEADS = 8
COLS = HEADS * HEAD
BQ = 256
BK = 512
STRIP = 512
DV = HEAD + 16

XRA, XLA, XRB, XLB, RR, RL, Q1A, Q2A, Q1B, Q2B, Q3A, Q3B, D1, D2, D3, D4, D5, D6 = range(18)
KR, KL, VR, VL, KRR, VLL = range(6)
S0A, S0B, S1A, S1B, S2, S3 = range(6)
PLAN = ((1, 0, S1A, 2), (1, 2, S1B, 2), (1, 2, S0B, 3), (1, 2, S0A, 4), (2, 2, S2, 2), (2, 2, S0B, 4), (4, 0, S3, 2), (4, 0, S1A, 3),
        (4, 1, S1A, 4), (4, 1, S1B, 3), (4, 1, S0A, 5), (5, 0, S0A, 8), (5, 0, S1B, 4), (5, 0, S2, 3), (5, 0, S0A, 7), (5, 2, S0B, 7),
        (5, 2, S0A, 6), (6, 0, S0B, 5), (6, 0, S0B, 6), (6, 2, S2, 4), (7, 0, S1A, 5), (7, 2, S3, 3), (8, 0, S1A, 7), (8, 1, S1B, 7),
        (9, 0, S1A, 8), (9, 0, S1A, 6), (9, 2, S1B, 5), (10, 0, S3, 4), (11, 0, S1B, 6), (12, 0, S0B, 8), (12, 0, S2, 5), (12, 1, S2, 7),
        (13, 0, S2, 6), (13, 2, S1B, 8), (14, 0, S2, 8), (14, 2, S3, 5), (15, 0, S3, 7), (16, 0, S3, 6), (16, 0, S3, 8))
LIGHT = (1,)


def _dot(a, b, ca, cb):
    return lax.dot_general(a, b, (((ca,), (cb,)), ((), ())), preferred_element_type=jnp.float32)


def _kernel(chunks, kv_heads, speed_ref, gain_ref, x_ref, wq_ref, wk_ref, wv_ref, wo_ref, seen_ref, wof_ref,
            a_s, wq_s, cos_s, sin_s, k_s, v_s, q_s, xin, sout, top_s, mix_s, s_s, ss, rs, kss, krs, xsem, osem, lsem, wsem, bsem):
    own = x_ref.shape[0]
    deep = wq_ref.shape[0]
    dp, me = lax.axis_index("dp"), lax.axis_index("sp")
    n = lax.axis_size("sp")
    right, left, far = lax.rem(me + 1, n), lax.rem(me + n - 1, n), lax.rem(me + 2, n)
    core = lax.rem(dp, 2)
    p = lax.rem(lax.div(dp, 2), 2)
    mate = {"dp": dp + 1 - 2 * core, "sp": me}
    pair = {"dp": dp + 2 - 4 * p, "sp": me}
    to_right, to_left = {"dp": dp, "sp": right}, {"dp": dp, "sp": left}
    half, quarter = deep // 2, deep // 8

    kvw = wk_ref.shape[1]
    rounds = 1 + 2 * chunks

    def place(r, shard, row, size):
        at = pl.ds(pl.multiple_of(shard * deep + row, 128), size)
        if r == 0:
            return wq_s.at[chunks - 1, at, pl.ds(0, 2 * kvw)]
        if r <= chunks:
            return wq_s.at[r - 1, at, :]
        return wof_ref.at[at, pl.ds((r - 1 - chunks) * COLS, COLS)]

    def source(r, row, size):
        if r == 0:
            return place(r, me, row, size)
        at = pl.ds(pl.multiple_of(row, 128), size)
        c = (r - 1) % chunks
        return (wq_ref if r <= chunks else wo_ref).at[at, pl.ds(c * COLS, COLS)]

    def kinds_of(r):
        return [kind for kind in range(18) if r in LIGHT or kind not in (Q1B, Q2B)]

    def copy(r, kind, arriving=False):
        b, pp = core * half, p
        if arriving and kind in (Q1A, Q2A, Q1B, Q2B, Q3A, Q3B):
            pp = 1 - p
        if arriving and kind >= D1:
            b = (1 - core) * half
        light = r in LIGHT
        edge, inner = (3 * pp, 1), (1 + pp, 1)
        mine, others = (2 * pp, 2), (2 * (1 - pp), 2)
        (first, size), shard, to = {
            XRA: (edge, left if arriving else me, to_right),
            XLA: (edge, right if arriving else me, to_left),
            XRB: (inner if light else (1, 2), left if arriving else me, to_right),
            XLB: (inner if light else (1, 2), right if arriving else me, to_left),
            RR: (inner, far if arriving else left, to_right),
            RL: (edge, far if arriving else right, to_left),
            Q1A: (edge, left, pair),
            Q2A: (edge, right, pair),
            Q1B: (inner, left, pair),
            Q2B: (inner, right, pair),
            Q3A: (inner, far, pair),
            Q3B: (edge, far, pair),
            D1: (mine if light else (pp, 3), left, mate),
            D2: (mine if light else (pp, 3), right, mate),
            D3: (others if light else (3 * (1 - pp), 1), left, mate),
            D4: (others if light else (3 * (1 - pp), 1), right, mate),
            D5: (mine, far, mate),
            D6: (others, far, mate),
        }[kind]
        row, size = b + first * quarter, size * quarter
        dst = place(r, shard, row, size)
        src = source(r, row, size) if kind <= XLB and not arriving else dst
        return pltpu.make_async_remote_copy(src_ref=src, dst_ref=dst, send_sem=ss.at[r, kind], recv_sem=rs.at[r, kind],
                                            device_id=to, device_id_type=MESH)

    def start(r, *kinds):
        for kind in kinds:
            if kind in kinds_of(r):
                copy(r, kind).start()

    def arrive(r, *kinds):
        for kind in kinds:
            if kind in kinds_of(r):
                copy(r, kind, True).wait_recv()

    def sent(r):
        for kind in kinds_of(r):
            copy(r, kind).wait_send()

    def s0a(r):
        start(r, XRA, XLA)

    def s0b(r):
        start(r, XRB, XLB)

    def s0(r):
        s0a(r)
        s0b(r)

    def s1a(r):
        arrive(r, XRA)
        start(r, Q1A)
        arrive(r, XLA)
        start(r, Q2A, RL)

    def s1b(r):
        arrive(r, XRB)
        start(r, RR, Q1B, D1)
        arrive(r, XLB)
        start(r, Q2B, D2)

    def s2(r):
        arrive(r, RL)
        start(r, Q3B)
        arrive(r, RR)
        start(r, Q3A, D5)
        arrive(r, Q1A, Q2A, Q1B, Q2B)
        start(r, D3, D4)

    def s3(r):
        arrive(r, Q3A, Q3B)
        start(r, D6)

    def s4(r):
        arrive(r, D1, D2, D3, D4, D5, D6)

    def kv_copy(kind, arriving=False):
        shard = {KR: left if arriving else me, KL: right if arriving else me, VR: left if arriving else me,
                 VL: right if arriving else me, KRR: far if arriving else left, VLL: far if arriving else right}[kind]
        to = to_right if kind in (KR, VR, KRR) else to_left
        at = pl.ds(pl.multiple_of(shard * own, 128), own)
        ref = k_s.at[:, at, :] if kind in (KR, KL, KRR) else v_s.at[:, pl.ds(0, HEAD), at]
        return pltpu.make_async_remote_copy(src_ref=ref, dst_ref=ref, send_sem=kss.at[kind], recv_sem=krs.at[kind],
                                            device_id=to, device_id_type=MESH)

    mine = pl.ds(pl.multiple_of(me * deep, 128), deep)
    wk_in = pltpu.make_async_copy(wk_ref, wq_s.at[chunks - 1, mine, pl.ds(0, kvw)], lsem.at[0])
    wv_in = pltpu.make_async_copy(wv_ref, wq_s.at[chunks - 1, mine, pl.ds(kvw, kvw)], lsem.at[1])
    wk_in.start()
    wv_in.start()
    rows = xin.shape[1]
    x_in = [pltpu.make_async_copy(x_ref.at[pl.ds(i * rows, rows), :], xin.at[i % 2], xsem.at[i % 2]) for i in range(own // rows)]
    x_in[0].start()
    x_in[1].start()
    barrier = pltpu.get_barrier_semaphore()
    for other in (mate, pair, to_right, to_left):
        pl.semaphore_signal(barrier, inc=1, device_id=other, device_id_type=MESH)
    pl.semaphore_wait(barrier, 4)

    wk_in.wait()
    wv_in.wait()
    s0(0)
    wq_in = [pltpu.make_async_copy(wq_ref.at[:, pl.ds(c * COLS, COLS)], wq_s.at[c, mine, :], wsem.at[c]) for c in range(chunks)]
    for w in wq_in[:-1]:
        w.start()

    for i, block in enumerate(x_in):
        block.wait()
        wide = xin[i % 2].astype(jnp.float32)
        scale = lax.rsqrt(jnp.mean(wide * wide, -1, keepdims=True) + 1e-6)
        a_s[i * rows : (i + 1) * rows, :] = (wide * scale * gain_ref[...].astype(jnp.float32)[None]).astype(jnp.bfloat16)
        if i + 2 < len(x_in):
            x_in[i + 2].start()
        if i == len(x_in) // 2:
            s1a(0)
    for h in range(kv_heads):
        v_s[h, HEAD:, :] = jnp.ones((DV - HEAD, v_s.shape[2]), jnp.bfloat16)

    s1b(0)
    s0(1)

    def tables(i, _):
        at = pl.ds(pl.multiple_of(i * 128, 128), 128)
        place = (me * own + i * 128 + lax.broadcasted_iota(jnp.int32, (128, HEAD), 0)).astype(jnp.float32)
        angle = place * speed_ref[...]
        sine = jnp.sin(angle)
        cos_s[at, :] = jnp.cos(angle)
        sin_s[at, :] = jnp.where(lax.broadcasted_iota(jnp.int32, (128, HEAD), 1) < HEAD // 2, -sine, sine)
        return _

    lax.fori_loop(0, own // 128, tables, None)
    s2(0)
    s3(0)
    s1a(1)
    s4(0)
    s1b(1)

    def turn(t, at):
        wide = t.astype(jnp.bfloat16).astype(jnp.float32)
        return (wide * cos_s[at, :] + pltpu.roll(wide, HEAD // 2, 1) * sin_s[at, :]).astype(jnp.bfloat16)

    def keys_values(i, _):
        at = pl.ds(pl.multiple_of(i * BQ, BQ), BQ)
        there = pl.ds(pl.multiple_of(me * own + i * BQ, BQ), BQ)
        kv = _dot(a_s[at, :], wq_s[chunks - 1, :, : 2 * kvw], 1, 0)
        for h in range(kv_heads):
            k_s[h, there, :] = turn(kv[:, h * HEAD : (h + 1) * HEAD], at)
            v_s[h, :HEAD, there] = kv[:, kvw + h * HEAD : kvw + (h + 1) * HEAD].astype(jnp.bfloat16).T
        return _

    lax.fori_loop(0, own // BQ, keys_values, None)
    sent(0)
    wq_in[-1].start()

    for kind in (KR, VL, VR, KL):
        kv_copy(kind).start()
    s2(1)
    s3(1)
    s4(1)
    wq_in[0].wait()

    group = 2
    tall = own // 2

    def project(c):
        def tile(i, _):
            m, j = lax.div(i, HEADS // group), lax.rem(i, HEADS // group)
            at = pl.ds(pl.multiple_of(m * tall, tall), tall)
            cols = pl.ds(pl.multiple_of(j * group * HEAD, group * HEAD), group * HEAD)
            q = _dot(a_s[at, :], wq_s[c, :, cols], 1, 0)
            for h in range(group):
                q_s[j * group + h, at, :] = turn(q[:, h * HEAD : (h + 1) * HEAD], at)
            return _

        lax.fori_loop(0, 2 * (HEADS // group), tile, None)

    e = HEAD**-0.5 * LOG2E
    wide = HEADS * BQ
    strips = list(range(0, wide, STRIP))

    def attend(c, qb, between):
        g = lax.div(c * kv_heads, chunks)
        first = me * own + qb * BQ

        def queries(i):
            return q_s[:, pl.ds(pl.multiple_of(i * BQ, BQ), BQ), :].reshape(wide, HEAD)

        q = queries(qb)
        top_s[...] = jnp.full(top_s.shape, NEG, jnp.float32)
        mix_s[...] = jnp.zeros(mix_s.shape, jnp.float32)

        def scores(j, at, q):
            s_s[:, at : at + STRIP] = _dot(k_s[g, pl.ds(pl.multiple_of(j * BK, BK), BK), :], q[at : at + STRIP], 1, 1)

        def block(j, size, last):
            values = v_s[g, :, pl.ds(pl.multiple_of(j * BK, BK), size)]
            if last:
                gap = lax.rem(lax.broadcasted_iota(jnp.int32, (size, STRIP), 1), BQ) - lax.broadcasted_iota(jnp.int32, (size, STRIP), 0)
                ok = gap >= j * BK - first
            for at in strips:
                s = s_s[:size, at : at + STRIP]
                if last:
                    s = jnp.where(ok, s, HIDDEN)
                old = top_s[:, at : at + STRIP]
                top = jnp.maximum(old, s.max(axis=0, keepdims=True))
                top_s[:, at : at + STRIP] = top
                w, keep = jnp.exp2((s - top) * e).astype(jnp.bfloat16), jnp.exp2((old - top) * e)
                if last:
                    scores(0, at, later)
                else:
                    scores(j + 1, at, q)
                mix_s[:, at : at + STRIP] = mix_s[:, at : at + STRIP] * keep + _dot(values, w, 1, 0)

        whole = lax.div(first + 1, BK)
        later = queries(lax.rem(qb + 1, own // BQ))

        @pl.when(qb == 0)
        def _():
            for at in strips:
                scores(0, at, q)

        lax.fori_loop(0, whole, lambda j, _: block(j, BK, False), None)
        between()

        @pl.when(lax.rem(qb, 2) == 0)
        def _():
            block(whole, BQ, True)

        @pl.when(lax.rem(qb, 2) == 1)
        def _():
            block(whole, BK, True)

    steps = own // BQ

    def out_copy(t):
        c, qb, slot = lax.div(t, steps), lax.rem(t, steps), lax.rem(t, 2)
        return pltpu.make_async_copy(sout.at[slot], seen_ref.at[pl.ds(pl.multiple_of(qb * BQ, BQ), BQ), pl.ds(pl.multiple_of(c * COLS, COLS), COLS)],
                                     osem.at[slot])

    bounce = [pltpu.make_async_copy(wo_ref.at[:, pl.ds(c * COLS, COLS)], wq_s.at[0, pl.ds(c * deep, deep), :], bsem.at[c]) for c in range(chunks)]
    settle = [pltpu.make_async_copy(wq_s.at[0, pl.ds(c * deep, deep), :], wof_ref.at[mine, pl.ds(c * COLS, COLS)], lsem.at[c])
              for c in range(chunks)]

    end = chunks * steps
    todo = {}
    for t, part, stage, r in PLAN:
        todo.setdefault((t, part), []).append(functools.partial((s0a, s0b, s1a, s1b, s2, s3)[stage], r))
    for c in range(1, chunks):
        todo.setdefault((steps * c, 0), []).extend([functools.partial(s4, 1 + c), wq_in[c].wait])

    def before():
        sent(1)
        for w in bounce:
            w.start()

    def after():
        for w in bounce:
            w.wait()
        for w in settle:
            w.start()

    todo.setdefault((steps + 1, 0), []).append(before)
    todo.setdefault((steps + 3, 0), []).append(after)

    def links(t, part):
        for (at, where), jobs in todo.items():
            if where == part and at < end:
                @pl.when(t == at)
                def _():
                    for job in jobs:
                        job()

    def body(t, _):
        c, qb, slot = lax.div(t, steps), lax.rem(t, steps), lax.rem(t, 2)
        links(t, 0)

        @pl.when((qb == 0) & (c > 0))
        def _():
            project(c)

        links(t, 1)
        attend(c, qb, functools.partial(links, t, 2))

        @pl.when(t >= 2)
        def _():
            out_copy(t - 2).wait()

        for h in range(HEADS):
            at = slice(h * BQ, (h + 1) * BQ)
            part = mix_s[:HEAD, at] * (1 / mix_s[HEAD : HEAD + 1, at])
            sout[slot, :, h * HEAD : (h + 1) * HEAD] = part.T.astype(jnp.bfloat16)
        out_copy(t).start()

    kv_copy(KR, True).wait_recv()
    kv_copy(KRR).start()
    kv_copy(VL, True).wait_recv()
    kv_copy(VLL).start()
    s0(2)
    s0a(3)
    project(0)
    for kind in (KL, VR, KRR, VLL):
        kv_copy(kind, True).wait_recv()
    lax.fori_loop(0, chunks * steps, body, None)

    for job in todo.get((end, 0), []):
        job()
    for r in range(1 + chunks, rounds):
        s4(r)
    for r in range(2, rounds):
        sent(r)
    for kind in range(6):
        kv_copy(kind).wait_send()
    for w in settle:
        w.wait()
    out_copy(chunks * steps - 2).wait()
    out_copy(chunks * steps - 1).wait()


def solution(mesh):
    def step(x, gain, wq, wk, wv, wo):
        own, d = x.shape
        deep, width = wq.shape
        kvw = wk.shape[1]
        n = d // deep
        chunks, kv_heads = width // COLS, kvw // HEAD
        half = HEAD // 2
        speed = THETA ** (-jnp.arange(half, dtype=jnp.float32) / half)
        speed = jnp.concatenate([speed, speed])[None]
        anywhere, vmem = pl.BlockSpec(memory_space=pl.ANY), pl.BlockSpec(memory_space=pltpu.VMEM)
        rounds = 1 + 2 * chunks
        seen, wo = pl.pallas_call(
            functools.partial(_kernel, chunks, kv_heads),
            out_shape=[jax.ShapeDtypeStruct((own, width), jnp.bfloat16), jax.ShapeDtypeStruct((n * deep, d), jnp.bfloat16)],
            in_specs=[vmem] * 2 + [anywhere] * 5,
            out_specs=[anywhere] * 2,
            scratch_shapes=[
                pltpu.VMEM((own, d), jnp.bfloat16),
                pltpu.VMEM((chunks, n * deep, COLS), jnp.bfloat16),
                pltpu.VMEM((own, HEAD), jnp.float32),
                pltpu.VMEM((own, HEAD), jnp.float32),
                pltpu.VMEM((kv_heads, n * own, HEAD), jnp.bfloat16),
                pltpu.VMEM((kv_heads, DV, n * own), jnp.bfloat16),
                pltpu.VMEM((HEADS, own, HEAD), jnp.bfloat16),
                pltpu.VMEM((2, 128, d), jnp.bfloat16),
                pltpu.VMEM((2, BQ, COLS), jnp.bfloat16),
                pltpu.VMEM((1, HEADS * BQ), jnp.float32),
                pltpu.VMEM((DV, HEADS * BQ), jnp.float32),
                pltpu.VMEM((BK, HEADS * BQ), jnp.float32),
                pltpu.SemaphoreType.DMA((rounds, 18)),
                pltpu.SemaphoreType.DMA((rounds, 18)),
                pltpu.SemaphoreType.DMA((6,)),
                pltpu.SemaphoreType.DMA((6,)),
                pltpu.SemaphoreType.DMA((2,)),
                pltpu.SemaphoreType.DMA((2,)),
                pltpu.SemaphoreType.DMA((max(chunks, 2),)),
                pltpu.SemaphoreType.DMA((chunks,)),
                pltpu.SemaphoreType.DMA((chunks,)),
            ],
            compiler_params=pltpu.CompilerParams(collective_id=0, has_side_effects=True, vmem_limit_bytes=VMEM),
        )(speed, gain, x, wq, wk, wv, wo)
        y = jnp.dot(seen, wo, preferred_element_type=jnp.float32)
        return (x.astype(jnp.float32) + y).astype(jnp.bfloat16)

    tokens, whole = P(("dp", "sp"), None), P("sp", None)
    return jax.shard_map(
        step,
        mesh=mesh,
        in_specs=(tokens, P(None), whole, whole, whole, whole),
        out_specs=tokens,
        check_vma=False,
    )
```

```python
import functools

import jax
import jax.numpy as jnp
from jax import lax
from jax.experimental import pallas as pl
from jax.experimental.pallas import tpu as pltpu
from jax.sharding import PartitionSpec as P

HEAD = 128
THETA = 10000
NEG = -1e30
HIDDEN = 2 * NEG
LOG2E = 1.4426950408889634
VMEM = 67043328
MESH = pl.DeviceIdType.MESH

HEADS = 8
COLS = HEADS * HEAD
BQ = 256
BK = 512
STRIP = 512
DV = HEAD + 16

XRA, XLA, XRB, XLB, RR, RL, Q1A, Q2A, Q1B, Q2B, Q3A, Q3B, D1, D2, D3, D4, D5, D6 = range(18)
KR, KL, VR, VL, KRR, VLL = range(6)
S0A, S0B, S1A, S1B, S2, S3 = range(6)
PLAN = ((1, 0, S1A, 2), (1, 2, S1B, 2), (2, 0, S0B, 3), (2, 2, S2, 2), (2, 2, S0A, 6), (3, 0, S1A, 3), (3, 2, S1B, 3), (3, 2, S0A, 4),
        (4, 0, S3, 2), (4, 0, S0B, 6), (4, 1, S2, 3), (5, 0, S0B, 4), (5, 0, S1A, 6), (5, 2, S1A, 4), (5, 2, S1B, 6), (6, 0, S3, 3),
        (6, 2, S1B, 4), (7, 0, S0A, 7), (7, 0, S0A, 5), (7, 0, S0B, 5), (7, 2, S0A, 8), (7, 2, S2, 6), (8, 0, S2, 4), (8, 2, S0B, 7),
        (8, 2, S1A, 5), (9, 0, S1A, 7), (9, 2, S1B, 5), (10, 0, S0B, 8), (10, 2, S1A, 8), (11, 0, S3, 4), (12, 0, S2, 5),
        (12, 1, S1B, 7), (12, 2, S1B, 8), (13, 0, S2, 7), (14, 0, S2, 8), (14, 0, S3, 5), (15, 0, S3, 7), (15, 2, S3, 6), (16, 0, S3, 8))
LIGHT = (1,)


def _dot(a, b, ca, cb):
    return lax.dot_general(a, b, (((ca,), (cb,)), ((), ())), preferred_element_type=jnp.float32)


def _kernel(chunks, kv_heads, speed_ref, gain_ref, x_ref, wq_ref, wk_ref, wv_ref, wo_ref, seen_ref, wof_ref,
            a_s, wq_s, cos_s, sin_s, k_s, v_s, q_s, xin, sout, top_s, mix_s, s_s, ss, rs, kss, krs, xsem, osem, lsem, wsem, bsem):
    own = x_ref.shape[0]
    deep = wq_ref.shape[0]
    dp, me = lax.axis_index("dp"), lax.axis_index("sp")
    n = lax.axis_size("sp")
    right, left, far = lax.rem(me + 1, n), lax.rem(me + n - 1, n), lax.rem(me + 2, n)
    core = lax.rem(dp, 2)
    p = lax.rem(lax.div(dp, 2), 2)
    mate = {"dp": dp + 1 - 2 * core, "sp": me}
    pair = {"dp": dp + 2 - 4 * p, "sp": me}
    to_right, to_left = {"dp": dp, "sp": right}, {"dp": dp, "sp": left}
    half, quarter = deep // 2, deep // 8

    kvw = wk_ref.shape[1]
    rounds = 1 + 2 * chunks

    def place(r, shard, row, size):
        at = pl.ds(pl.multiple_of(shard * deep + row, 128), size)
        if r == 0:
            return wq_s.at[chunks - 1, at, pl.ds(0, 2 * kvw)]
        if r <= chunks:
            return wq_s.at[r - 1, at, :]
        return wof_ref.at[at, pl.ds((r - 1 - chunks) * COLS, COLS)]

    def source(r, row, size):
        if r == 0:
            return place(r, me, row, size)
        at = pl.ds(pl.multiple_of(row, 128), size)
        c = (r - 1) % chunks
        return (wq_ref if r <= chunks else wo_ref).at[at, pl.ds(c * COLS, COLS)]

    def kinds_of(r):
        return [kind for kind in range(18) if r in LIGHT or kind not in (Q1B, Q2B)]

    def copy(r, kind, arriving=False):
        b, pp = core * half, p
        if arriving and kind in (Q1A, Q2A, Q1B, Q2B, Q3A, Q3B):
            pp = 1 - p
        if arriving and kind >= D1:
            b = (1 - core) * half
        light = r in LIGHT
        edge, inner = (3 * pp, 1), (1 + pp, 1)
        mine, others = (2 * pp, 2), (2 * (1 - pp), 2)
        (first, size), shard, to = {
            XRA: (edge, left if arriving else me, to_right),
            XLA: (edge, right if arriving else me, to_left),
            XRB: (inner if light else (1, 2), left if arriving else me, to_right),
            XLB: (inner if light else (1, 2), right if arriving else me, to_left),
            RR: (inner, far if arriving else left, to_right),
            RL: (edge, far if arriving else right, to_left),
            Q1A: (edge, left, pair),
            Q2A: (edge, right, pair),
            Q1B: (inner, left, pair),
            Q2B: (inner, right, pair),
            Q3A: (inner, far, pair),
            Q3B: (edge, far, pair),
            D1: (mine if light else (pp, 3), left, mate),
            D2: (mine if light else (pp, 3), right, mate),
            D3: (others if light else (3 * (1 - pp), 1), left, mate),
            D4: (others if light else (3 * (1 - pp), 1), right, mate),
            D5: (mine, far, mate),
            D6: (others, far, mate),
        }[kind]
        row, size = b + first * quarter, size * quarter
        dst = place(r, shard, row, size)
        src = source(r, row, size) if kind <= XLB and not arriving else dst
        return pltpu.make_async_remote_copy(src_ref=src, dst_ref=dst, send_sem=ss.at[r, kind], recv_sem=rs.at[r, kind],
                                            device_id=to, device_id_type=MESH)

    def start(r, *kinds):
        for kind in kinds:
            if kind in kinds_of(r):
                copy(r, kind).start()

    def arrive(r, *kinds):
        for kind in kinds:
            if kind in kinds_of(r):
                copy(r, kind, True).wait_recv()

    def sent(r):
        for kind in kinds_of(r):
            copy(r, kind).wait_send()

    def s0a(r):
        start(r, XRA, XLA)

    def s0b(r):
        start(r, XRB, XLB)

    def s0(r):
        s0a(r)
        s0b(r)

    def s1a(r):
        arrive(r, XRA)
        start(r, Q1A)
        arrive(r, XLA)
        start(r, Q2A, RL)

    def s1b(r):
        arrive(r, XRB)
        start(r, RR, Q1B, D1)
        arrive(r, XLB)
        start(r, Q2B, D2)

    def s2(r):
        arrive(r, RL)
        start(r, Q3B)
        arrive(r, RR)
        start(r, Q3A, D5)
        arrive(r, Q1A, Q2A, Q1B, Q2B)
        start(r, D3, D4)

    def s3(r):
        arrive(r, Q3A, Q3B)
        start(r, D6)

    def s4(r):
        arrive(r, D1, D2, D3, D4, D5, D6)

    def kv_copy(kind, arriving=False):
        shard = {KR: left if arriving else me, KL: right if arriving else me, VR: left if arriving else me,
                 VL: right if arriving else me, KRR: far if arriving else left, VLL: far if arriving else right}[kind]
        to = to_right if kind in (KR, VR, KRR) else to_left
        at = pl.ds(pl.multiple_of(shard * own, 128), own)
        ref = k_s.at[:, at, :] if kind in (KR, KL, KRR) else v_s.at[:, pl.ds(0, HEAD), at]
        return pltpu.make_async_remote_copy(src_ref=ref, dst_ref=ref, send_sem=kss.at[kind], recv_sem=krs.at[kind],
                                            device_id=to, device_id_type=MESH)

    mine = pl.ds(pl.multiple_of(me * deep, 128), deep)
    wk_in = pltpu.make_async_copy(wk_ref, wq_s.at[chunks - 1, mine, pl.ds(0, kvw)], lsem.at[0])
    wv_in = pltpu.make_async_copy(wv_ref, wq_s.at[chunks - 1, mine, pl.ds(kvw, kvw)], lsem.at[1])
    wk_in.start()
    wv_in.start()
    rows = xin.shape[1]
    x_in = [pltpu.make_async_copy(x_ref.at[pl.ds(i * rows, rows), :], xin.at[i % 2], xsem.at[i % 2]) for i in range(own // rows)]
    x_in[0].start()
    x_in[1].start()
    barrier = pltpu.get_barrier_semaphore()
    for other in (mate, pair, to_right, to_left):
        pl.semaphore_signal(barrier, inc=1, device_id=other, device_id_type=MESH)
    pl.semaphore_wait(barrier, 4)

    wk_in.wait()
    wv_in.wait()
    s0(0)
    wq_in = [pltpu.make_async_copy(wq_ref.at[:, pl.ds(c * COLS, COLS)], wq_s.at[c, mine, :], wsem.at[c]) for c in range(chunks)]
    for w in wq_in[:-1]:
        w.start()

    for i, block in enumerate(x_in):
        block.wait()
        wide = xin[i % 2].astype(jnp.float32)
        scale = lax.rsqrt(jnp.mean(wide * wide, -1, keepdims=True) + 1e-6)
        a_s[i * rows : (i + 1) * rows, :] = (wide * scale * gain_ref[...].astype(jnp.float32)[None]).astype(jnp.bfloat16)
        if i + 2 < len(x_in):
            x_in[i + 2].start()
        if i == len(x_in) // 2:
            s1a(0)
    for h in range(kv_heads):
        v_s[h, HEAD:, :] = jnp.ones((DV - HEAD, v_s.shape[2]), jnp.bfloat16)

    s1b(0)
    s0(1)

    def tables(i, _):
        at = pl.ds(pl.multiple_of(i * 128, 128), 128)
        place = (me * own + i * 128 + lax.broadcasted_iota(jnp.int32, (128, HEAD), 0)).astype(jnp.float32)
        angle = place * speed_ref[...]
        sine = jnp.sin(angle)
        cos_s[at, :] = jnp.cos(angle)
        sin_s[at, :] = jnp.where(lax.broadcasted_iota(jnp.int32, (128, HEAD), 1) < HEAD // 2, -sine, sine)
        return _

    lax.fori_loop(0, own // 128, tables, None)
    s2(0)
    s3(0)
    s1a(1)
    s4(0)
    s1b(1)

    def turn(t, at):
        wide = t.astype(jnp.bfloat16).astype(jnp.float32)
        return (wide * cos_s[at, :] + pltpu.roll(wide, HEAD // 2, 1) * sin_s[at, :]).astype(jnp.bfloat16)

    def keys_values(i, _):
        at = pl.ds(pl.multiple_of(i * BQ, BQ), BQ)
        there = pl.ds(pl.multiple_of(me * own + i * BQ, BQ), BQ)
        kv = _dot(a_s[at, :], wq_s[chunks - 1, :, : 2 * kvw], 1, 0)
        for h in range(kv_heads):
            k_s[h, there, :] = turn(kv[:, h * HEAD : (h + 1) * HEAD], at)
            v_s[h, :HEAD, there] = kv[:, kvw + h * HEAD : kvw + (h + 1) * HEAD].astype(jnp.bfloat16).T
        return _

    lax.fori_loop(0, own // BQ, keys_values, None)
    sent(0)
    wq_in[-1].start()

    for kind in (KR, VL, VR, KL):
        kv_copy(kind).start()
    s2(1)
    s3(1)
    s4(1)
    wq_in[0].wait()

    group = 2
    tall = own // 2

    def project(c):
        def tile(i, _):
            m, j = lax.div(i, HEADS // group), lax.rem(i, HEADS // group)
            at = pl.ds(pl.multiple_of(m * tall, tall), tall)
            cols = pl.ds(pl.multiple_of(j * group * HEAD, group * HEAD), group * HEAD)
            q = _dot(a_s[at, :], wq_s[c, :, cols], 1, 0)
            for h in range(group):
                q_s[j * group + h, at, :] = turn(q[:, h * HEAD : (h + 1) * HEAD], at)
            return _

        lax.fori_loop(0, 2 * (HEADS // group), tile, None)

    e = HEAD**-0.5 * LOG2E
    wide = HEADS * BQ
    strips = list(range(0, wide, STRIP))

    def attend(c, qb, between):
        g = lax.div(c * kv_heads, chunks)
        first = me * own + qb * BQ

        def queries(i):
            return q_s[:, pl.ds(pl.multiple_of(i * BQ, BQ), BQ), :].reshape(wide, HEAD)

        q = queries(qb)
        top_s[...] = jnp.full(top_s.shape, NEG, jnp.float32)
        mix_s[...] = jnp.zeros(mix_s.shape, jnp.float32)

        def scores(j, at, q):
            s_s[:, at : at + STRIP] = _dot(k_s[g, pl.ds(pl.multiple_of(j * BK, BK), BK), :], q[at : at + STRIP], 1, 1)

        def block(j, size, last):
            values = v_s[g, :, pl.ds(pl.multiple_of(j * BK, BK), size)]
            if last:
                gap = lax.rem(lax.broadcasted_iota(jnp.int32, (size, STRIP), 1), BQ) - lax.broadcasted_iota(jnp.int32, (size, STRIP), 0)
                ok = gap >= j * BK - first
            for at in strips:
                s = s_s[:size, at : at + STRIP]
                if last:
                    s = jnp.where(ok, s, HIDDEN)
                old = top_s[:, at : at + STRIP]
                top = jnp.maximum(old, s.max(axis=0, keepdims=True))
                top_s[:, at : at + STRIP] = top
                w, keep = jnp.exp2((s - top) * e).astype(jnp.bfloat16), jnp.exp2((old - top) * e)
                if last:
                    scores(0, at, later)
                else:
                    scores(j + 1, at, q)
                mix_s[:, at : at + STRIP] = mix_s[:, at : at + STRIP] * keep + _dot(values, w, 1, 0)

        whole = lax.div(first + 1, BK)
        later = queries(lax.rem(qb + 1, own // BQ))

        @pl.when(qb == 0)
        def _():
            for at in strips:
                scores(0, at, q)

        lax.fori_loop(0, whole, lambda j, _: block(j, BK, False), None)
        between()

        @pl.when(lax.rem(qb, 2) == 0)
        def _():
            block(whole, BQ, True)

        @pl.when(lax.rem(qb, 2) == 1)
        def _():
            block(whole, BK, True)

    steps = own // BQ

    def out_copy(t):
        c, qb, slot = lax.div(t, steps), lax.rem(t, steps), lax.rem(t, 2)
        return pltpu.make_async_copy(sout.at[slot], seen_ref.at[pl.ds(pl.multiple_of(qb * BQ, BQ), BQ), pl.ds(pl.multiple_of(c * COLS, COLS), COLS)],
                                     osem.at[slot])

    bounce = [pltpu.make_async_copy(wo_ref.at[:, pl.ds(c * COLS, COLS)], wq_s.at[0, pl.ds(c * deep, deep), :], bsem.at[c]) for c in range(chunks)]
    settle = [pltpu.make_async_copy(wq_s.at[0, pl.ds(c * deep, deep), :], wof_ref.at[mine, pl.ds(c * COLS, COLS)], lsem.at[c])
              for c in range(chunks)]

    end = chunks * steps
    todo = {}
    for t, part, stage, r in PLAN:
        todo.setdefault((t, part), []).append(functools.partial((s0a, s0b, s1a, s1b, s2, s3)[stage], r))
    for c in range(1, chunks):
        todo.setdefault((steps * c, 0), []).extend([functools.partial(s4, 1 + c), wq_in[c].wait])

    def before():
        sent(1)
        for w in bounce:
            w.start()

    def after():
        for w in bounce:
            w.wait()
        for w in settle:
            w.start()

    todo.setdefault((steps + 1, 0), []).append(before)
    todo.setdefault((steps + 3, 0), []).append(after)

    def links(t, part):
        for (at, where), jobs in todo.items():
            if where == part and at < end:
                @pl.when(t == at)
                def _():
                    for job in jobs:
                        job()

    def body(t, _):
        c, qb, slot = lax.div(t, steps), lax.rem(t, steps), lax.rem(t, 2)
        links(t, 0)

        @pl.when((qb == 0) & (c > 0))
        def _():
            project(c)

        links(t, 1)
        attend(c, qb, functools.partial(links, t, 2))

        @pl.when(t >= 2)
        def _():
            out_copy(t - 2).wait()

        for h in range(HEADS):
            at = slice(h * BQ, (h + 1) * BQ)
            part = mix_s[:HEAD, at] * (1 / mix_s[HEAD : HEAD + 1, at])
            sout[slot, :, h * HEAD : (h + 1) * HEAD] = part.T.astype(jnp.bfloat16)
        out_copy(t).start()

    kv_copy(KR, True).wait_recv()
    kv_copy(KRR).start()
    kv_copy(VL, True).wait_recv()
    kv_copy(VLL).start()
    s0(2)
    s0a(3)
    project(0)
    for kind in (KL, VR, KRR, VLL):
        kv_copy(kind, True).wait_recv()
    lax.fori_loop(0, chunks * steps, body, None)

    for job in todo.get((end, 0), []):
        job()
    for r in range(1 + chunks, rounds):
        s4(r)
    for r in range(2, rounds):
        sent(r)
    for kind in range(6):
        kv_copy(kind).wait_send()
    for w in settle:
        w.wait()
    out_copy(chunks * steps - 2).wait()
    out_copy(chunks * steps - 1).wait()


def solution(mesh):
    def step(x, gain, wq, wk, wv, wo):
        own, d = x.shape
        deep, width = wq.shape
        kvw = wk.shape[1]
        n = d // deep
        chunks, kv_heads = width // COLS, kvw // HEAD
        half = HEAD // 2
        speed = THETA ** (-jnp.arange(half, dtype=jnp.float32) / half)
        speed = jnp.concatenate([speed, speed])[None]
        anywhere, vmem = pl.BlockSpec(memory_space=pl.ANY), pl.BlockSpec(memory_space=pltpu.VMEM)
        rounds = 1 + 2 * chunks
        seen, wo = pl.pallas_call(
            functools.partial(_kernel, chunks, kv_heads),
            out_shape=[jax.ShapeDtypeStruct((own, width), jnp.bfloat16), jax.ShapeDtypeStruct((n * deep, d), jnp.bfloat16)],
            in_specs=[vmem] * 2 + [anywhere] * 5,
            out_specs=[anywhere] * 2,
            scratch_shapes=[
                pltpu.VMEM((own, d), jnp.bfloat16),
                pltpu.VMEM((chunks, n * deep, COLS), jnp.bfloat16),
                pltpu.VMEM((own, HEAD), jnp.float32),
                pltpu.VMEM((own, HEAD), jnp.float32),
                pltpu.VMEM((kv_heads, n * own, HEAD), jnp.bfloat16),
                pltpu.VMEM((kv_heads, DV, n * own), jnp.bfloat16),
                pltpu.VMEM((HEADS, own, HEAD), jnp.bfloat16),
                pltpu.VMEM((2, 128, d), jnp.bfloat16),
                pltpu.VMEM((2, BQ, COLS), jnp.bfloat16),
                pltpu.VMEM((1, HEADS * BQ), jnp.float32),
                pltpu.VMEM((DV, HEADS * BQ), jnp.float32),
                pltpu.VMEM((BK, HEADS * BQ), jnp.float32),
                pltpu.SemaphoreType.DMA((rounds, 18)),
                pltpu.SemaphoreType.DMA((rounds, 18)),
                pltpu.SemaphoreType.DMA((6,)),
                pltpu.SemaphoreType.DMA((6,)),
                pltpu.SemaphoreType.DMA((2,)),
                pltpu.SemaphoreType.DMA((2,)),
                pltpu.SemaphoreType.DMA((max(chunks, 2),)),
                pltpu.SemaphoreType.DMA((chunks,)),
                pltpu.SemaphoreType.DMA((chunks,)),
            ],
            compiler_params=pltpu.CompilerParams(collective_id=0, has_side_effects=True, vmem_limit_bytes=VMEM),
        )(speed, gain, x, wq, wk, wv, wo)
        y = jnp.dot(seen, wo, preferred_element_type=jnp.float32)
        return (x.astype(jnp.float32) + y).astype(jnp.bfloat16)

    tokens, whole = P(("dp", "sp"), None), P("sp", None)
    return jax.shard_map(
        step,
        mesh=mesh,
        in_specs=(tokens, P(None), whole, whole, whole, whole),
        out_specs=tokens,
        check_vma=False,
    )
```
